32 devices in a mesh: row: 4 (over y, x), col: 8 (over z, core).
Axes of the slice: x: 2, y: 2, z: 4, core: 2. Of those that a mesh axis runs over, the one named last changes fastest.
Arguments:
- pair: float32 [512, 512, 128], P('row', 'col'), may hold values from -6 to 6
- in_gain: float32 [2, 128], replicated, may hold values from 1 to 4
- in_bias: float32 [2, 128], replicated, may hold values from -1.5 to 1.5
- proj_weight: bfloat16 [2, 128, 640], replicated, may hold values from -0.5 to 0.5
- proj_bias: float32 [2, 640], replicated, may hold values from -1.5 to 1.5
- mid_gain: float32 [2, 128], replicated, may hold values from 0.5 to 2
- mid_bias: float32 [2, 128], replicated, may hold values from -3 to 3
- out_weight: bfloat16 [2, 128, 128], replicated, may hold values from -0.5 to 0.5
- out_bias: float32 [2, 128], replicated, may hold values from -3 to 3
Outputs:
- updated: float32 [512, 512, 128], P('row', 'col')
The draws below stay inside these ranges and needn't reach their ends.
All inputs are finite; a program needn't handle non-finite values.
Results may differ from the reference program's by a relative error of at most 0.015.
Values may be sent and summed in bfloat16 or wider, within the bound.
A program may use at most 128 MiB of HBM per device.

```python
import math
import jax
import jax.numpy as jnp
from jax import lax

C = 128
HID = 128
N = 512


def shard_levels(rng, shape, shards, smallest, top_value):
    def one(dim, blocks):
        heights = jax.random.uniform(jax.random.fold_in(jax.random.fold_in(rng, 6), dim), (blocks,), jnp.float32, smallest / len(shards), top_value / len(shards))
        return jnp.repeat(jnp.exp(heights), shape[dim] // blocks).reshape((-1,) + (1,) * (len(shape) - dim - 1))

    level = one(*shards[0])
    for cut in shards[1:]:
        level = level * one(*cut)
    return level


def noise(key, extent, scale, limit, cuts=(), held_as=jnp.bfloat16):
    drawn = jax.random.normal(key, extent, jnp.float32) * scale
    if len(cuts) > 0:
        drawn = shard_levels(key, extent, cuts, -0.22, 0.18) * drawn
    return jnp.clip(drawn, min=-limit, max=limit).astype(held_as)


def setup_inputs(seed: int = 0) -> dict:
    arg_keys = jax.random.split(jax.random.key(seed), 10)
    return {
        "pair": noise(arg_keys[0], (N, N, C), 1.0, 6.0, ((0, 4), (1, 8)), jnp.float32),
        "in_gain": jnp.clip(jnp.exp(jax.random.uniform(arg_keys[1], (2, C), jnp.float32, math.log(1.0), math.log(4.0))), 1.0, 4.0),
        "in_bias": noise(arg_keys[2], (2, C), 0.25, 1.5, (), jnp.float32),
        "proj_weight": noise(arg_keys[3], (2, C, 4 * HID + C), C ** -0.5, 0.5),
        "proj_bias": noise(arg_keys[4], (2, 4 * HID + C), 0.25, 1.5, (), jnp.float32),
        "mid_gain": jnp.clip(jnp.exp(jax.random.uniform(arg_keys[5], (2, HID), jnp.float32, math.log(0.5), math.log(2.0))), 0.5, 2.0),
        "mid_bias": noise(arg_keys[6], (2, HID), 0.5, 3.0, (), jnp.float32),
        "out_weight": noise(arg_keys[7], (2, HID, C), HID ** -0.5, 0.5),
        "out_bias": noise(arg_keys[8], (2, C), 0.5, 3.0, (), jnp.float32),
    }


def layer_norm(values, gain, offset):
    mean = lax.optimization_barrier(jnp.mean(values, -1, keepdims=True))
    centred = values - mean
    variance = lax.optimization_barrier(jnp.mean(centred * centred, -1, keepdims=True))
    return centred * lax.rsqrt(variance + 1e-05) * gain + offset

def reference(pair, in_gain, in_bias, proj_weight, proj_bias, mid_gain, mid_bias, out_weight, out_bias):
    hidden = out_weight.shape[1]
    state = pair
    for update in range(2):
        normed = layer_norm(state, in_gain[update], in_bias[update]).astype(jnp.bfloat16)
        proj = jnp.dot(normed, proj_weight[update], preferred_element_type=jnp.float32) + proj_bias[update]
        left = (jax.nn.sigmoid(proj[..., hidden:2 * hidden]) * proj[..., 0:hidden]).astype(jnp.bfloat16)
        right = (jax.nn.sigmoid(proj[..., 3 * hidden:4 * hidden]) * proj[..., 2 * hidden:3 * hidden]).astype(jnp.bfloat16)
        gate = jax.nn.sigmoid(proj[..., 4 * hidden:])
        if update == 0:
            mixed = jnp.einsum('ikc,jkc->ijc', left.astype(jnp.float32), right.astype(jnp.float32))
        else:
            mixed = jnp.einsum('kic,kjc->ijc', left.astype(jnp.float32), right.astype(jnp.float32))
        middle = layer_norm(mixed, mid_gain[update], mid_bias[update]).astype(jnp.bfloat16)
        outcome = jnp.dot(middle, out_weight[update], preferred_element_type=jnp.float32) + out_bias[update]
        state = state + gate * outcome
    return state
```

```python
import functools

import jax
import jax.numpy as jnp
from jax import lax
from jax.experimental import pallas as pl
from jax.experimental.pallas import tpu as pltpu
from jax.sharding import PartitionSpec as P

MESH = pl.DeviceIdType.MESH


def triangle_kernel(
    update, rows, cols, left_ref, right_ref, out_ref, left_all, right_all, mixed_all,
    send_sem, recv_sem, back_send_sem, back_recv_sem, local_sem,
):
    devices = rows * cols
    row, col = lax.axis_index("row"), lax.axis_index("col")
    me = row * cols + col

    def place(offset):
        other = lax.rem(me + offset, devices)
        return other, lax.div(other, cols), lax.rem(other, cols)

    barrier = pltpu.get_barrier_semaphore()

    def greet(offset, carry):
        _, r, c = place(offset)
        pl.semaphore_signal(barrier, inc=1, device_id=(r, c), device_id_type=MESH)
        return carry

    lax.fori_loop(1, devices, greet, 0)
    pl.semaphore_wait(barrier, devices - 1)

    pairs = ((left_ref, left_all), (right_ref, right_all))

    def outgoing(which, offset):
        source, target = pairs[which]
        other, r, c = place(offset)
        return pltpu.make_async_remote_copy(
            src_ref=source.at[other],
            dst_ref=target.at[row, col],
            send_sem=send_sem.at[which, other],
            recv_sem=recv_sem.at[which, me],
            device_id=(r, c),
            device_id_type=MESH,
        )

    def incoming(which, offset):
        source, target = pairs[which]
        other, r, c = place(offset)
        return pltpu.make_async_remote_copy(
            src_ref=source.at[other],
            dst_ref=target.at[r, c],
            send_sem=send_sem.at[which, other],
            recv_sem=recv_sem.at[which, other],
            device_id=(r, c),
            device_id_type=MESH,
        )

    def send(offset, carry):
        outgoing(0, offset).start()
        outgoing(1, offset).start()
        return carry

    lax.fori_loop(1, devices, send, 0)
    own = [
        pltpu.make_async_copy(source.at[me], target.at[row, col], local_sem.at[which])
        for which, (source, target) in enumerate(pairs)
    ]
    for copy in own:
        copy.start()
    for copy in own:
        copy.wait()

    def receive(offset, carry):
        incoming(0, offset).wait_recv()
        incoming(1, offset).wait_recv()
        return carry

    lax.fori_loop(1, devices, receive, 0)

    channels, depth, width = left_all.shape[2:]

    def whole(ref, channel):
        return jnp.concatenate(
            [ref[r, :, channel].reshape(cols * depth, width) for r in range(rows)], axis=1
        )

    def product(channel, carry):
        contract = ((0,), (0,)) if update == 0 else ((1,), (1,))
        mixed = lax.dot_general(
            whole(right_all, channel),
            whole(left_all, channel),
            (contract, ((), ())),
            preferred_element_type=jnp.float32,
        ).astype(jnp.bfloat16)
        for r in range(rows):
            mixed_all[r, :, channel] = mixed[:, r * width : (r + 1) * width].reshape(
                cols, depth, width
            )
        return carry

    lax.fori_loop(0, channels, product, 0)

    def outgoing_back(offset):
        other, r, c = place(offset)
        return pltpu.make_async_remote_copy(
            src_ref=mixed_all.at[r, c],
            dst_ref=out_ref.at[me],
            send_sem=back_send_sem.at[other],
            recv_sem=back_recv_sem.at[me],
            device_id=(r, c),
            device_id_type=MESH,
        )

    def incoming_back(offset):
        other, r, c = place(offset)
        return pltpu.make_async_remote_copy(
            src_ref=mixed_all.at[r, c],
            dst_ref=out_ref.at[other],
            send_sem=back_send_sem.at[other],
            recv_sem=back_recv_sem.at[other],
            device_id=(r, c),
            device_id_type=MESH,
        )

    def send_back(offset, carry):
        outgoing_back(offset).start()
        return carry

    lax.fori_loop(1, devices, send_back, 0)
    last = pltpu.make_async_copy(mixed_all.at[row, col], out_ref.at[me], local_sem.at[0])
    last.start()
    last.wait()

    def finish_all(offset, carry):
        incoming_back(offset).wait_recv()
        outgoing_back(offset).wait_send()
        outgoing(0, offset).wait_send()
        outgoing(1, offset).wait_send()
        return carry

    lax.fori_loop(1, devices, finish_all, 0)


def triangle(update, rows, cols, left, right):
    devices = rows * cols
    channels, depth, width = left.shape
    split = (devices, channels // devices, depth, width)
    held = (rows, cols) + split[1:]
    anywhere = pl.BlockSpec(memory_space=pl.ANY)
    mixed = pl.pallas_call(
        functools.partial(triangle_kernel, update, rows, cols),
        out_shape=jax.ShapeDtypeStruct(split, jnp.bfloat16),
        in_specs=[anywhere] * 2,
        out_specs=anywhere,
        scratch_shapes=[
            pltpu.VMEM(held, jnp.bfloat16),
            pltpu.VMEM(held, jnp.bfloat16),
            pltpu.VMEM(held, jnp.bfloat16),
            pltpu.SemaphoreType.DMA((2, devices)),
            pltpu.SemaphoreType.DMA((2, devices)),
            pltpu.SemaphoreType.DMA((devices,)),
            pltpu.SemaphoreType.DMA((devices,)),
            pltpu.SemaphoreType.DMA((2,)),
        ],
        compiler_params=pltpu.CompilerParams(
            collective_id=update, has_side_effects=True, vmem_limit_bytes=32 * 1024 * 1024
        ),
        name=f"triangle_{update}",
    )(left.reshape(split), right.reshape(split))
    return mixed.reshape(left.shape)


def layer_norm(values, gain, offset):
    mean = jnp.mean(values, -1, keepdims=True)
    centred = values - mean
    variance = jnp.mean(centred * centred, -1, keepdims=True)
    return centred * lax.rsqrt(variance + 1e-05) * gain + offset


def projections(state, update, in_gain, in_bias, proj_weight, proj_bias):
    hidden = (proj_weight.shape[2] - state.shape[2]) // 4
    normed = layer_norm(state, in_gain[update], in_bias[update]).astype(jnp.bfloat16)
    proj = (
        jnp.dot(normed, proj_weight[update], preferred_element_type=jnp.float32) + proj_bias[update]
    )
    left = (jax.nn.sigmoid(proj[..., hidden : 2 * hidden]) * proj[..., 0:hidden]).astype(
        jnp.bfloat16
    )
    right = (
        jax.nn.sigmoid(proj[..., 3 * hidden : 4 * hidden]) * proj[..., 2 * hidden : 3 * hidden]
    ).astype(jnp.bfloat16)
    gate = jax.nn.sigmoid(proj[..., 4 * hidden :])
    left_major = jnp.transpose(left, (2, 0, 1))
    right_major = jnp.transpose(right, (2, 0, 1))
    return (left_major, right_major, gate)


def finish(state, mixed_major, gate, update, mid_gain, mid_bias, out_weight, out_bias):
    mixed = jnp.transpose(mixed_major, (1, 2, 0))
    middle = layer_norm(mixed, mid_gain[update], mid_bias[update]).astype(jnp.bfloat16)
    outcome = (
        jnp.dot(middle, out_weight[update], preferred_element_type=jnp.float32) + out_bias[update]
    )
    return state + gate * outcome


def body(pair, in_gain, in_bias, proj_weight, proj_bias, mid_gain, mid_bias, out_weight, out_bias):
    left, right, gate = projections(pair, 0, in_gain, in_bias, proj_weight, proj_bias)
    terms = jnp.einsum(
        "cjk,cik->cji",
        lax.all_gather(right, "row", axis=1, tiled=True),
        left,
        preferred_element_type=jnp.float32,
    )
    summed = lax.psum_scatter(
        terms.astype(jnp.bfloat16), "col", scatter_dimension=1, tiled=True
    ).astype(jnp.float32)
    mixed = jnp.transpose(summed, (0, 2, 1))
    state = finish(pair, mixed, gate, 0, mid_gain, mid_bias, out_weight, out_bias)
    left, right, gate = projections(state, 1, in_gain, in_bias, proj_weight, proj_bias)
    terms = jnp.einsum(
        "cki,ckj->cij",
        lax.all_gather(left, "col", axis=2, tiled=True),
        right,
        preferred_element_type=jnp.float32,
    )
    mixed = lax.psum_scatter(
        terms.astype(jnp.bfloat16), "row", scatter_dimension=1, tiled=True
    ).astype(jnp.float32)
    return finish(state, mixed, gate, 1, mid_gain, mid_bias, out_weight, out_bias)


def channel_body(
    rows, cols, pair, in_gain, in_bias, proj_weight, proj_bias, mid_gain, mid_bias, out_weight,
    out_bias,
):
    state = pair
    for update in range(2):
        left, right, gate = projections(state, update, in_gain, in_bias, proj_weight, proj_bias)
        mixed = triangle(
            update, rows, cols, jnp.transpose(left, (0, 2, 1)), jnp.transpose(right, (0, 2, 1))
        )
        mixed = jnp.transpose(mixed.astype(jnp.float32), (0, 2, 1))
        state = finish(state, mixed, gate, update, mid_gain, mid_bias, out_weight, out_bias)
    return state


def solution(mesh):
    placed = (P("row", "col", None), P(), P(), P(), P(), P(), P(), P(), P())
    rows, cols = mesh.shape["row"], mesh.shape["col"]

    def run(*arrays):
        hidden = arrays[7].shape[1]
        local = functools.partial(channel_body, rows, cols)
        if hidden % (rows * cols) != 0:
            local = body
        return jax.shard_map(
            local, mesh=mesh, in_specs=placed, out_specs=P("row", "col", None), check_vma=False
        )(*arrays)

    return run
```

```python
import functools

import jax
import jax.numpy as jnp
from jax import lax
from jax.experimental import pallas as pl
from jax.experimental.pallas import tpu as pltpu
from jax.sharding import PartitionSpec as P

MESH = pl.DeviceIdType.MESH


def triangle_kernel(
    update, rows, cols, left_ref, right_ref, out_ref, left_all, right_all, mixed_all,
    send_sem, recv_sem, back_send_sem, back_recv_sem, local_sem,
):
    devices = rows * cols
    row, col = lax.axis_index("row"), lax.axis_index("col")
    me = row * cols + col

    def place(offset):
        other = lax.rem(me + offset, devices)
        return other, lax.div(other, cols), lax.rem(other, cols)

    barrier = pltpu.get_barrier_semaphore()

    def greet(offset, carry):
        _, r, c = place(offset)
        pl.semaphore_signal(barrier, inc=1, device_id=(r, c), device_id_type=MESH)
        return carry

    lax.fori_loop(1, devices, greet, 0)
    pl.semaphore_wait(barrier, devices - 1)

    pairs = ((left_ref, left_all), (right_ref, right_all))

    def outgoing(which, offset):
        source, target = pairs[which]
        other, r, c = place(offset)
        return pltpu.make_async_remote_copy(
            src_ref=source.at[other],
            dst_ref=target.at[row, col],
            send_sem=send_sem.at[which, other],
            recv_sem=recv_sem.at[which, me],
            device_id=(r, c),
            device_id_type=MESH,
        )

    def incoming(which, offset):
        source, target = pairs[which]
        other, r, c = place(offset)
        return pltpu.make_async_remote_copy(
            src_ref=source.at[other],
            dst_ref=target.at[r, c],
            send_sem=send_sem.at[which, other],
            recv_sem=recv_sem.at[which, other],
            device_id=(r, c),
            device_id_type=MESH,
        )

    def send(offset, carry):
        outgoing(0, offset).start()
        outgoing(1, offset).start()
        return carry

    lax.fori_loop(1, devices, send, 0)
    own = [
        pltpu.make_async_copy(source.at[me], target.at[row, col], local_sem.at[which])
        for which, (source, target) in enumerate(pairs)
    ]
    for copy in own:
        copy.start()
    for copy in own:
        copy.wait()

    def receive(offset, carry):
        incoming(0, offset).wait_recv()
        incoming(1, offset).wait_recv()
        return carry

    lax.fori_loop(1, devices, receive, 0)

    channels, depth, width = left_all.shape[2:]

    def whole(ref, channel):
        return jnp.concatenate(
            [ref[r, :, channel].reshape(cols * depth, width) for r in range(rows)], axis=1
        )

    def product(channel, carry):
        contract = ((0,), (0,)) if update == 0 else ((1,), (1,))
        mixed = lax.dot_general(
            whole(right_all, channel),
            whole(left_all, channel),
            (contract, ((), ())),
            preferred_element_type=jnp.float32,
        ).astype(jnp.bfloat16)
        for r in range(rows):
            mixed_all[r, :, channel] = mixed[:, r * width : (r + 1) * width].reshape(
                cols, depth, width
            )
        return carry

    lax.fori_loop(0, channels, product, 0)

    def outgoing_back(offset):
        other, r, c = place(offset)
        return pltpu.make_async_remote_copy(
            src_ref=mixed_all.at[r, c],
            dst_ref=out_ref.at[me],
            send_sem=back_send_sem.at[other],
            recv_sem=back_recv_sem.at[me],
            device_id=(r, c),
            device_id_type=MESH,
        )

    def incoming_back(offset):
        other, r, c = place(offset)
        return pltpu.make_async_remote_copy(
            src_ref=mixed_all.at[r, c],
            dst_ref=out_ref.at[other],
            send_sem=back_send_sem.at[other],
            recv_sem=back_recv_sem.at[other],
            device_id=(r, c),
            device_id_type=MESH,
        )

    def send_back(offset, carry):
        outgoing_back(offset).start()
        return carry

    lax.fori_loop(1, devices, send_back, 0)
    last = pltpu.make_async_copy(mixed_all.at[row, col], out_ref.at[me], local_sem.at[0])
    last.start()
    last.wait()

    def finish_all(offset, carry):
        incoming_back(offset).wait_recv()
        outgoing_back(offset).wait_send()
        outgoing(0, offset).wait_send()
        outgoing(1, offset).wait_send()
        return carry

    lax.fori_loop(1, devices, finish_all, 0)


def triangle(update, rows, cols, left, right):
    devices = rows * cols
    channels, depth, width = left.shape
    split = (devices, channels // devices, depth, width)
    held = (rows, cols) + split[1:]
    anywhere = pl.BlockSpec(memory_space=pl.ANY)
    mixed = pl.pallas_call(
        functools.partial(triangle_kernel, update, rows, cols),
        out_shape=jax.ShapeDtypeStruct(split, jnp.bfloat16),
        in_specs=[anywhere] * 2,
        out_specs=anywhere,
        scratch_shapes=[
            pltpu.VMEM(held, jnp.bfloat16),
            pltpu.VMEM(held, jnp.bfloat16),
            pltpu.VMEM(held, jnp.bfloat16),
            pltpu.SemaphoreType.DMA((2, devices)),
            pltpu.SemaphoreType.DMA((2, devices)),
            pltpu.SemaphoreType.DMA((devices,)),
            pltpu.SemaphoreType.DMA((devices,)),
            pltpu.SemaphoreType.DMA((2,)),
        ],
        compiler_params=pltpu.CompilerParams(
            collective_id=update, has_side_effects=True, vmem_limit_bytes=32 * 1024 * 1024
        ),
        name=f"triangle_{update}",
    )(left.reshape(split), right.reshape(split))
    return mixed.reshape(left.shape)


def layer_norm(values, gain, offset):
    mean = jnp.mean(values, -1, keepdims=True)
    centred = values - mean
    variance = jnp.mean(centred * centred, -1, keepdims=True)
    return centred * lax.rsqrt(variance + 1e-05) * gain + offset


def projections(state, update, in_gain, in_bias, proj_weight, proj_bias):
    hidden = (proj_weight.shape[2] - state.shape[2]) // 4
    normed = layer_norm(state, in_gain[update], in_bias[update]).astype(jnp.bfloat16)
    proj = (
        jnp.dot(normed, proj_weight[update], preferred_element_type=jnp.float32) + proj_bias[update]
    )
    left = (jax.nn.sigmoid(proj[..., hidden : 2 * hidden]) * proj[..., 0:hidden]).astype(
        jnp.bfloat16
    )
    right = (
        jax.nn.sigmoid(proj[..., 3 * hidden : 4 * hidden]) * proj[..., 2 * hidden : 3 * hidden]
    ).astype(jnp.bfloat16)
    gate = jax.nn.sigmoid(proj[..., 4 * hidden :])
    left_major = jnp.transpose(left, (2, 0, 1))
    right_major = jnp.transpose(right, (2, 0, 1))
    return (left_major, right_major, gate)


def finish(state, mixed_major, gate, update, mid_gain, mid_bias, out_weight, out_bias):
    mixed = jnp.transpose(mixed_major, (1, 2, 0))
    middle = layer_norm(mixed, mid_gain[update], mid_bias[update]).astype(jnp.bfloat16)
    outcome = (
        jnp.dot(middle, out_weight[update], preferred_element_type=jnp.float32) + out_bias[update]
    )
    return state + gate * outcome


def body(pair, in_gain, in_bias, proj_weight, proj_bias, mid_gain, mid_bias, out_weight, out_bias):
    left, right, gate = projections(pair, 0, in_gain, in_bias, proj_weight, proj_bias)
    terms = jnp.einsum(
        "cjk,cik->cji",
        lax.all_gather(right, "row", axis=1, tiled=True),
        left,
        preferred_element_type=jnp.float32,
    )
    summed = lax.psum_scatter(
        terms.astype(jnp.bfloat16), "col", scatter_dimension=1, tiled=True
    ).astype(jnp.float32)
    mixed = jnp.transpose(summed, (0, 2, 1))
    state = finish(pair, mixed, gate, 0, mid_gain, mid_bias, out_weight, out_bias)
    left, right, gate = projections(state, 1, in_gain, in_bias, proj_weight, proj_bias)
    terms = jnp.einsum(
        "cki,ckj->cij",
        lax.all_gather(left, "col", axis=2, tiled=True),
        right,
        preferred_element_type=jnp.float32,
    )
    mixed = lax.psum_scatter(
        terms.astype(jnp.bfloat16), "row", scatter_dimension=1, tiled=True
    ).astype(jnp.float32)
    return finish(state, mixed, gate, 1, mid_gain, mid_bias, out_weight, out_bias)


CHUNK = 16


def take(ref, b):
    n, chunk, m = ref.shape
    return ref.reshape(n * chunk, m)[pl.ds(b, n, stride=chunk), :]


def put(ref, b, value):
    n, chunk, m = ref.shape
    ref.reshape(n * chunk, m)[pl.ds(b, n, stride=chunk), :] = value


def project_plane(plane, gain, offset, weights_t, bias_t, gate_weight, gate_bias):
    normed = layer_norm(plane, gain, offset).astype(jnp.bfloat16)
    proj_t = (
        lax.dot_general(
            weights_t, normed, (((1,), (1,)), ((), ())), preferred_element_type=jnp.float32
        )
        + bias_t
    )
    hidden = proj_t.shape[0] // 4
    parts = [proj_t[n * hidden : (n + 1) * hidden] for n in range(4)]
    gate = jax.nn.sigmoid(
        jnp.dot(normed, gate_weight, preferred_element_type=jnp.float32) + gate_bias
    )
    return jax.nn.sigmoid(parts[1]) * parts[0], jax.nn.sigmoid(parts[3]) * parts[2], gate


def finish_plane(plane, mixed, gate, gain_t, offset_t, weight, bias):
    mean = jnp.mean(mixed, 0, keepdims=True)
    centred = mixed - mean
    variance = jnp.mean(centred * centred, 0, keepdims=True)
    middle = (centred * lax.rsqrt(variance + 1e-05) * gain_t + offset_t).astype(jnp.bfloat16)
    outcome = (
        lax.dot_general(
            middle, weight, (((0,), (0,)), ((), ())), preferred_element_type=jnp.float32
        )
        + bias
    )
    return plane + gate * outcome


def first_kernel(pair_ref, *refs):
    before, (left_ref, right_ref, gate_ref, left_held, right_held) = refs[:6], refs[6:]

    def step(b, carry):
        left, right, gate = project_plane(take(pair_ref, b), *[ref[...] for ref in before])
        put(left_held, b, left)
        put(right_held, b, right)
        gate_ref[b] = gate
        return carry

    lax.fori_loop(0, CHUNK, step, 0, unroll=2)
    left_ref[...] = left_held[...].astype(jnp.bfloat16)
    right_ref[...] = right_held[...].astype(jnp.bfloat16)


def middle_kernel(pair_ref, mixed_ref, old_gate_ref, *refs):
    after, before = refs[:4], refs[4:10]
    state_ref, left_ref, right_ref, gate_ref, left_held, right_held, mixed_held = refs[10:]
    mixed_held[...] = mixed_ref[...].astype(jnp.float32)

    def step(b, carry):
        state = finish_plane(
            take(pair_ref, b), take(mixed_held, b), old_gate_ref[b], *[ref[...] for ref in after]
        )
        state_ref[b] = state
        left, right, gate = project_plane(state, *[ref[...] for ref in before])
        put(left_held, b, left)
        put(right_held, b, right)
        gate_ref[b] = gate
        return carry

    lax.fori_loop(0, CHUNK, step, 0, unroll=2)
    left_ref[...] = left_held[...].astype(jnp.bfloat16)
    right_ref[...] = right_held[...].astype(jnp.bfloat16)


def last_kernel(state_ref, mixed_ref, gate_ref, *refs):
    after, (out_ref, mixed_held) = refs[:4], refs[4:]
    mixed_held[...] = mixed_ref[...].astype(jnp.float32)

    def step(b, carry):
        put(
            out_ref,
            b,
            finish_plane(
                state_ref[b], take(mixed_held, b), gate_ref[b], *[ref[...] for ref in after]
            ),
        )
        return carry

    lax.fori_loop(0, CHUNK, step, 0, unroll=2)


def pointwise(kernel, name, depth, streams, constants, outs, held):
    def spec(shape, where):
        block = tuple(CHUNK if n == where else extent for n, extent in enumerate(shape))
        return pl.BlockSpec(block, lambda i: tuple(i if n == where else 0 for n in range(3)))

    def fixed(array):
        return pl.BlockSpec(array.shape, lambda i: (0,) * array.ndim)

    return pl.pallas_call(
        kernel,
        grid=(depth // CHUNK,),
        out_shape=[shape for shape, _ in outs],
        in_specs=[spec(array.shape, where) for array, where in streams]
        + [fixed(array) for array in constants],
        out_specs=[spec(shape.shape, where) for shape, where in outs],
        scratch_shapes=[pltpu.VMEM(shape, jnp.float32) for shape in held],
        compiler_params=pltpu.CompilerParams(vmem_limit_bytes=48 * 1024 * 1024),
        name=name,
    )(*[array for array, _ in streams], *constants)


def channel_body(
    rows, cols, pair, in_gain, in_bias, proj_weight, proj_bias, mid_gain, mid_bias, out_weight,
    out_bias,
):
    width, depth, wide = pair.shape
    hidden = out_weight.shape[1]

    def before(update):
        weight, bias = proj_weight[update], proj_bias[update]
        return [
            in_gain[update][None],
            in_bias[update][None],
            weight[:, : 4 * hidden].T,
            jnp.broadcast_to(bias[: 4 * hidden, None], (4 * hidden, width)),
            weight[:, 4 * hidden :],
            bias[None, 4 * hidden :],
        ]

    def after(update):
        return [
            jnp.broadcast_to(mid_gain[update][:, None], (hidden, width)),
            jnp.broadcast_to(mid_bias[update][:, None], (hidden, width)),
            out_weight[update],
            out_bias[update][None],
        ]

    major = (jax.ShapeDtypeStruct((hidden, depth, width), jnp.bfloat16), 1)
    planes = (jax.ShapeDtypeStruct((depth, width, wide), jnp.float32), 0)
    held = (hidden, CHUNK, width)
    left, right, gate = pointwise(
        first_kernel, "first", depth, [(pair, 1)], before(0), [major, major, planes], [held] * 2
    )
    mixed = triangle(0, rows, cols, left, right)
    state, left, right, gate = pointwise(
        middle_kernel, "middle", depth, [(pair, 1), (mixed, 1), (gate, 0)],
        after(0) + before(1), [planes, major, major, planes], [held] * 3,
    )
    mixed = triangle(1, rows, cols, left, right)
    (updated,) = pointwise(
        last_kernel, "last", depth, [(state, 0), (mixed, 1), (gate, 0)], after(1),
        [(jax.ShapeDtypeStruct(pair.shape, jnp.float32), 1)], [held],
    )
    return updated


def solution(mesh):
    placed = (P("row", "col", None), P(), P(), P(), P(), P(), P(), P(), P())
    rows, cols = mesh.shape["row"], mesh.shape["col"]

    def run(*arrays):
        hidden = arrays[7].shape[1]
        local = functools.partial(channel_body, rows, cols)
        depth = arrays[0].shape[1] // cols
        if hidden % (rows * cols) != 0 or depth % CHUNK != 0:
            local = body
        return jax.shard_map(
            local, mesh=mesh, in_specs=placed, out_specs=P("row", "col", None), check_vma=False
        )(*arrays)

    return run
```

```python
import functools

import jax
import jax.numpy as jnp
from jax import lax
from jax.experimental import pallas as pl
from jax.experimental.pallas import tpu as pltpu
from jax.sharding import PartitionSpec as P

MESH = pl.DeviceIdType.MESH


def triangle_kernel(
    update, rows, cols, left_ref, right_ref, out_ref, left_all, right_all, mixed_all,
    send_sem, recv_sem, back_send_sem, back_recv_sem, local_sem,
):
    devices = rows * cols
    row, col = lax.axis_index("row"), lax.axis_index("col")
    me = row * cols + col

    def place(offset):
        other = lax.rem(me + offset, devices)
        return other, lax.div(other, cols), lax.rem(other, cols)

    barrier = pltpu.get_barrier_semaphore()

    def greet(offset, carry):
        _, r, c = place(offset)
        pl.semaphore_signal(barrier, inc=1, device_id=(r, c), device_id_type=MESH)
        return carry

    lax.fori_loop(1, devices, greet, 0)
    pl.semaphore_wait(barrier, devices - 1)

    pairs = ((left_ref, left_all), (right_ref, right_all))

    def outgoing(which, offset):
        source, target = pairs[which]
        other, r, c = place(offset)
        return pltpu.make_async_remote_copy(
            src_ref=source.at[other],
            dst_ref=target.at[row, col],
            send_sem=send_sem.at[which, other],
            recv_sem=recv_sem.at[which, me],
            device_id=(r, c),
            device_id_type=MESH,
        )

    def incoming(which, offset):
        source, target = pairs[which]
        other, r, c = place(offset)
        return pltpu.make_async_remote_copy(
            src_ref=source.at[other],
            dst_ref=target.at[r, c],
            send_sem=send_sem.at[which, other],
            recv_sem=recv_sem.at[which, other],
            device_id=(r, c),
            device_id_type=MESH,
        )

    def send(offset, carry):
        outgoing(0, offset).start()
        outgoing(1, offset).start()
        return carry

    lax.fori_loop(1, devices, send, 0)
    own = [
        pltpu.make_async_copy(source.at[me], target.at[row, col], local_sem.at[which])
        for which, (source, target) in enumerate(pairs)
    ]
    for copy in own:
        copy.start()
    for copy in own:
        copy.wait()

    def receive(offset, carry):
        incoming(0, offset).wait_recv()
        incoming(1, offset).wait_recv()
        return carry

    lax.fori_loop(1, devices, receive, 0)

    channels, depth, width = left_all.shape[2:]

    def whole(ref, channel):
        return jnp.concatenate(
            [ref[r, :, channel].reshape(cols * depth, width) for r in range(rows)], axis=1
        )

    def product(channel, carry):
        contract = ((0,), (0,)) if update == 0 else ((1,), (1,))
        mixed = lax.dot_general(
            whole(right_all, channel),
            whole(left_all, channel),
            (contract, ((), ())),
            preferred_element_type=jnp.float32,
        ).astype(jnp.bfloat16)
        for r in range(rows):
            mixed_all[r, :, channel] = mixed[:, r * width : (r + 1) * width].reshape(
                cols, depth, width
            )
        return carry

    lax.fori_loop(0, channels, product, 0)

    def outgoing_back(offset):
        other, r, c = place(offset)
        return pltpu.make_async_remote_copy(
            src_ref=mixed_all.at[r, c],
            dst_ref=out_ref.at[me],
            send_sem=back_send_sem.at[other],
            recv_sem=back_recv_sem.at[me],
            device_id=(r, c),
            device_id_type=MESH,
        )

    def incoming_back(offset):
        other, r, c = place(offset)
        return pltpu.make_async_remote_copy(
            src_ref=mixed_all.at[r, c],
            dst_ref=out_ref.at[other],
            send_sem=back_send_sem.at[other],
            recv_sem=back_recv_sem.at[other],
            device_id=(r, c),
            device_id_type=MESH,
        )

    def send_back(offset, carry):
        outgoing_back(offset).start()
        return carry

    lax.fori_loop(1, devices, send_back, 0)
    last = pltpu.make_async_copy(mixed_all.at[row, col], out_ref.at[me], local_sem.at[0])
    last.start()
    last.wait()

    def finish_all(offset, carry):
        incoming_back(offset).wait_recv()
        outgoing_back(offset).wait_send()
        outgoing(0, offset).wait_send()
        outgoing(1, offset).wait_send()
        return carry

    lax.fori_loop(1, devices, finish_all, 0)


def triangle(update, rows, cols, left, right):
    devices = rows * cols
    channels, depth, width = left.shape
    split = (devices, channels // devices, depth, width)
    held = (rows, cols) + split[1:]
    anywhere = pl.BlockSpec(memory_space=pl.ANY)
    mixed = pl.pallas_call(
        functools.partial(triangle_kernel, update, rows, cols),
        out_shape=jax.ShapeDtypeStruct(split, jnp.bfloat16),
        in_specs=[anywhere] * 2,
        out_specs=anywhere,
        scratch_shapes=[
            pltpu.VMEM(held, jnp.bfloat16),
            pltpu.VMEM(held, jnp.bfloat16),
            pltpu.VMEM(held, jnp.bfloat16),
            pltpu.SemaphoreType.DMA((2, devices)),
            pltpu.SemaphoreType.DMA((2, devices)),
            pltpu.SemaphoreType.DMA((devices,)),
            pltpu.SemaphoreType.DMA((devices,)),
            pltpu.SemaphoreType.DMA((2,)),
        ],
        compiler_params=pltpu.CompilerParams(
            collective_id=update, has_side_effects=True, vmem_limit_bytes=32 * 1024 * 1024
        ),
        name=f"triangle_{update}",
    )(left.reshape(split), right.reshape(split))
    return mixed.reshape(left.shape)


def layer_norm(values, gain, offset):
    mean = jnp.mean(values, -1, keepdims=True)
    centred = values - mean
    variance = jnp.mean(centred * centred, -1, keepdims=True)
    return centred * lax.rsqrt(variance + 1e-05) * gain + offset


def projections(state, update, in_gain, in_bias, proj_weight, proj_bias):
    hidden = (proj_weight.shape[2] - state.shape[2]) // 4
    normed = layer_norm(state, in_gain[update], in_bias[update]).astype(jnp.bfloat16)
    proj = (
        jnp.dot(normed, proj_weight[update], preferred_element_type=jnp.float32) + proj_bias[update]
    )
    left = (jax.nn.sigmoid(proj[..., hidden : 2 * hidden]) * proj[..., 0:hidden]).astype(
        jnp.bfloat16
    )
    right = (
        jax.nn.sigmoid(proj[..., 3 * hidden : 4 * hidden]) * proj[..., 2 * hidden : 3 * hidden]
    ).astype(jnp.bfloat16)
    gate = jax.nn.sigmoid(proj[..., 4 * hidden :])
    left_major = jnp.transpose(left, (2, 0, 1))
    right_major = jnp.transpose(right, (2, 0, 1))
    return (left_major, right_major, gate)


def finish(state, mixed_major, gate, update, mid_gain, mid_bias, out_weight, out_bias):
    mixed = jnp.transpose(mixed_major, (1, 2, 0))
    middle = layer_norm(mixed, mid_gain[update], mid_bias[update]).astype(jnp.bfloat16)
    outcome = (
        jnp.dot(middle, out_weight[update], preferred_element_type=jnp.float32) + out_bias[update]
    )
    return state + gate * outcome


def body(pair, in_gain, in_bias, proj_weight, proj_bias, mid_gain, mid_bias, out_weight, out_bias):
    left, right, gate = projections(pair, 0, in_gain, in_bias, proj_weight, proj_bias)
    terms = jnp.einsum(
        "cjk,cik->cji",
        lax.all_gather(right, "row", axis=1, tiled=True),
        left,
        preferred_element_type=jnp.float32,
    )
    summed = lax.psum_scatter(
        terms.astype(jnp.bfloat16), "col", scatter_dimension=1, tiled=True
    ).astype(jnp.float32)
    mixed = jnp.transpose(summed, (0, 2, 1))
    state = finish(pair, mixed, gate, 0, mid_gain, mid_bias, out_weight, out_bias)
    left, right, gate = projections(state, 1, in_gain, in_bias, proj_weight, proj_bias)
    terms = jnp.einsum(
        "cki,ckj->cij",
        lax.all_gather(left, "col", axis=2, tiled=True),
        right,
        preferred_element_type=jnp.float32,
    )
    mixed = lax.psum_scatter(
        terms.astype(jnp.bfloat16), "row", scatter_dimension=1, tiled=True
    ).astype(jnp.float32)
    return finish(state, mixed, gate, 1, mid_gain, mid_bias, out_weight, out_bias)


CHUNK = 16
UNROLL = 16


def sigmoid(x):
    return 0.5 * jnp.tanh(0.5 * x) + 0.5


def take(ref, b):
    n, chunk, m = ref.shape
    return ref.reshape(n * chunk, m)[pl.ds(b, n, stride=chunk), :]


def put(ref, b, value):
    n, chunk, m = ref.shape
    ref.reshape(n * chunk, m)[pl.ds(b, n, stride=chunk), :] = value


def project_plane(plane, gain, offset, weights_t, bias_t, gate_weight, gate_bias):
    normed = layer_norm(plane, gain, offset).astype(jnp.bfloat16)
    proj_t = (
        lax.dot_general(
            weights_t, normed, (((1,), (1,)), ((), ())), preferred_element_type=jnp.float32
        )
        + bias_t
    )
    hidden = proj_t.shape[0] // 4
    parts = [proj_t[n * hidden : (n + 1) * hidden] for n in range(4)]
    gate = sigmoid(
        jnp.dot(normed, gate_weight, preferred_element_type=jnp.float32) + gate_bias
    )
    return sigmoid(parts[1]) * parts[0], sigmoid(parts[3]) * parts[2], gate


def finish_plane(plane, mixed, gate, gain_t, offset_t, weight, bias):
    mean = jnp.mean(mixed, 0, keepdims=True)
    centred = mixed - mean
    variance = jnp.mean(centred * centred, 0, keepdims=True)
    middle = (centred * lax.rsqrt(variance + 1e-05) * gain_t + offset_t).astype(jnp.bfloat16)
    outcome = (
        lax.dot_general(
            middle, weight, (((0,), (0,)), ((), ())), preferred_element_type=jnp.float32
        )
        + bias
    )
    return plane + gate * outcome


def first_kernel(pair_ref, *refs):
    before, (left_ref, right_ref, gate_ref, left_held, right_held) = refs[:6], refs[6:]

    def step(b, carry):
        left, right, gate = project_plane(take(pair_ref, b), *[ref[...] for ref in before])
        put(left_held, b, left)
        put(right_held, b, right)
        gate_ref[b] = gate
        return carry

    lax.fori_loop(0, CHUNK, step, 0, unroll=UNROLL)
    left_ref[...] = left_held[...].astype(jnp.bfloat16)
    right_ref[...] = right_held[...].astype(jnp.bfloat16)


def middle_kernel(pair_ref, mixed_ref, old_gate_ref, *refs):
    after, before = refs[:4], refs[4:10]
    state_ref, left_ref, right_ref, gate_ref, left_held, right_held, mixed_held = refs[10:]
    mixed_held[...] = mixed_ref[...].astype(jnp.float32)

    def step(b, carry):
        state = finish_plane(
            take(pair_ref, b), take(mixed_held, b), old_gate_ref[b], *[ref[...] for ref in after]
        )
        state_ref[b] = state
        left, right, gate = project_plane(state, *[ref[...] for ref in before])
        put(left_held, b, left)
        put(right_held, b, right)
        gate_ref[b] = gate
        return carry

    lax.fori_loop(0, CHUNK, step, 0, unroll=UNROLL)
    left_ref[...] = left_held[...].astype(jnp.bfloat16)
    right_ref[...] = right_held[...].astype(jnp.bfloat16)


def last_kernel(state_ref, mixed_ref, gate_ref, *refs):
    after, (out_ref, mixed_held) = refs[:4], refs[4:]
    mixed_held[...] = mixed_ref[...].astype(jnp.float32)

    def step(b, carry):
        put(
            out_ref,
            b,
            finish_plane(
                state_ref[b], take(mixed_held, b), gate_ref[b], *[ref[...] for ref in after]
            ),
        )
        return carry

    lax.fori_loop(0, CHUNK, step, 0, unroll=UNROLL)


def pointwise(kernel, name, depth, streams, constants, outs, held):
    def spec(shape, where):
        block = tuple(CHUNK if n == where else extent for n, extent in enumerate(shape))
        return pl.BlockSpec(block, lambda i: tuple(i if n == where else 0 for n in range(3)))

    def fixed(array):
        return pl.BlockSpec(array.shape, lambda i: (0,) * array.ndim)

    return pl.pallas_call(
        kernel,
        grid=(depth // CHUNK,),
        out_shape=[shape for shape, _ in outs],
        in_specs=[spec(array.shape, where) for array, where in streams]
        + [fixed(array) for array in constants],
        out_specs=[spec(shape.shape, where) for shape, where in outs],
        scratch_shapes=[pltpu.VMEM(shape, jnp.float32) for shape in held],
        compiler_params=pltpu.CompilerParams(vmem_limit_bytes=48 * 1024 * 1024),
        name=name,
    )(*[array for array, _ in streams], *constants)


def channel_body(
    rows, cols, pair, in_gain, in_bias, proj_weight, proj_bias, mid_gain, mid_bias, out_weight,
    out_bias,
):
    width, depth, wide = pair.shape
    hidden = out_weight.shape[1]

    def before(update):
        weight, bias = proj_weight[update], proj_bias[update]
        return [
            in_gain[update][None],
            in_bias[update][None],
            weight[:, : 4 * hidden].T,
            jnp.broadcast_to(bias[: 4 * hidden, None], (4 * hidden, width)),
            weight[:, 4 * hidden :],
            bias[None, 4 * hidden :],
        ]

    def after(update):
        return [
            jnp.broadcast_to(mid_gain[update][:, None], (hidden, width)),
            jnp.broadcast_to(mid_bias[update][:, None], (hidden, width)),
            out_weight[update],
            out_bias[update][None],
        ]

    major = (jax.ShapeDtypeStruct((hidden, depth, width), jnp.bfloat16), 1)
    planes = (jax.ShapeDtypeStruct((depth, width, wide), jnp.float32), 0)
    held = (hidden, CHUNK, width)
    left, right, gate = pointwise(
        first_kernel, "first", depth, [(pair, 1)], before(0), [major, major, planes], [held] * 2
    )
    mixed = triangle(0, rows, cols, left, right)
    state, left, right, gate = pointwise(
        middle_kernel, "middle", depth, [(pair, 1), (mixed, 1), (gate, 0)],
        after(0) + before(1), [planes, major, major, planes], [held] * 3,
    )
    mixed = triangle(1, rows, cols, left, right)
    (updated,) = pointwise(
        last_kernel, "last", depth, [(state, 0), (mixed, 1), (gate, 0)], after(1),
        [(jax.ShapeDtypeStruct(pair.shape, jnp.float32), 1)], [held],
    )
    return updated


def solution(mesh):
    placed = (P("row", "col", None), P(), P(), P(), P(), P(), P(), P(), P())
    rows, cols = mesh.shape["row"], mesh.shape["col"]

    def run(*arrays):
        hidden = arrays[7].shape[1]
        local = functools.partial(channel_body, rows, cols)
        depth = arrays[0].shape[1] // cols
        if hidden % (rows * cols) != 0 or depth % CHUNK != 0:
            local = body
        return jax.shard_map(
            local, mesh=mesh, in_specs=placed, out_specs=P("row", "col", None), check_vma=False
        )(*arrays)

    return run
```
